32 devices in a mesh: node: 4 (over z), chip: 8 (over y, x, core).
Axes of the slice: x: 2, y: 2, z: 4, core: 2. Of those that a mesh axis runs over, the one named last changes fastest.
Arguments:
- pooled_grad: bfloat16 [2048, 4, 256], P(('node', 'chip')), may hold values from -6 to 6
- grad_scale: bfloat16 [2048, 4], P(('node', 'chip')), may hold values from 0.049804688 to 1
- hot_slot: int32 [2048, 4, 2], P(('node', 'chip')), may hold values from 0 to 511
- send_index: int32 [32, 32, 128], P(('node', 'chip')), may hold values from 0 to 255, as said below
- recv_row: int32 [32, 32, 128], P(('node', 'chip')), may hold values from 0 to 4096, as said below
- cold_weight: float32 [4, 32768, 256], P(None, ('node', 'chip')), may hold values from -3 to 3
- cold_accum: float32 [4, 32768], P(None, ('node', 'chip')), may hold values from 0.5 to 8
- hot_weight: float32 [4, 512, 256], replicated, may hold values from -3 to 3
- hot_accum: float32 [4, 512], replicated, may hold values from 1 to 64
Outputs:
- cold_weight_new: float32 [4, 32768, 256], P(None, ('node', 'chip'))
- cold_accum_new: float32 [4, 32768], P(None, ('node', 'chip'))
- hot_weight_new: float32 [4, 512, 256], replicated
- hot_accum_new: float32 [4, 512], replicated
The draws below stay inside these ranges and needn't reach their ends.
Inputs may be any that keep to these rules, and one draw needn't show every extreme that they name: send_index and recv_row describe the same lookups: slot c from p to q is filled exactly when recv_row[q, p, c] < 4096, the filled slots of a pair come first, and the table in both entries agrees; some owners receive all 128 slots filled from every sender in every draw. `recv_row`: see send_index; empty slots hold 4096.
All inputs are finite; a program needn't handle non-finite values.
Results may differ from the reference program's by a relative error of at most 0.0003.
Values may be sent and summed in bfloat16 or wider, within the bound.
No kernel may reach another device: no remote copies, remote signals or barrier semaphores. Data moves between devices by JAX's collectives and lax.ppermute only.
A program may use at most 64 MiB of HBM per device.

```python
import math
import jax
import jax.numpy as jnp
import numpy as np
from jax import lax

D = 256
NT = 4
ROWS_DEV = 1024
B_DEV = 64
LH = 2
HOT = 512
CAP = 128
B = 2048
TABLE_ROWS = 32768
DEVICES = 32


def routing(key):
    keys = jax.random.split(jax.random.fold_in(key, 7), 7)
    order = jax.random.permutation(keys[0], DEVICES)
    heavy = order < max(1, DEVICES // 8)
    filled_count = jax.random.randint(keys[1], (DEVICES, DEVICES), max(1, CAP // 4), CAP // 2 + 1)
    filled_count = jnp.where(heavy[None, :], CAP, filled_count)
    filled = jnp.arange(CAP, dtype=jnp.int32)[None, None, :] < filled_count[:, :, None]
    sample = jax.random.randint(keys[2], (DEVICES, DEVICES, CAP), 0, B_DEV)
    table = jax.random.randint(keys[3], (DEVICES, DEVICES, CAP), 0, NT)
    first = jax.random.randint(keys[4], (DEVICES, DEVICES, CAP), 0, ROWS_DEV)
    second = jax.random.randint(keys[5], (DEVICES, DEVICES, CAP), 0, ROWS_DEV)
    third = jax.random.randint(keys[6], (DEVICES, DEVICES, CAP), 0, ROWS_DEV)
    row = jnp.minimum(jnp.minimum(first, second), third)
    return (filled, sample, table, row)


def draw_send_index(key, part):
    filled, sample, table, row = routing(key)
    return (sample * NT + table).astype(jnp.int32)


def draw_recv_row(key, part):
    filled, sample, table, row = routing(key)
    target = jnp.where(filled, table * ROWS_DEV + row, NT * ROWS_DEV)
    return jnp.transpose(target, (1, 0, 2)).astype(jnp.int32)


def touch_ends(result, stream_key, least, high):
    spot = [jax.random.randint(jax.random.fold_in(stream_key, axis), (), 0, length) for axis, length in enumerate(result.shape)]
    widest = result.shape.index(max(result.shape))
    neighbour = spot[:widest] + [(spot[widest] + 1) % result.shape[widest]] + spot[widest + 1:]
    return result.at[tuple(spot)].set(least).at[tuple(neighbour)].set(high)


def steps_of(stream_key, extent, cuts, low, top_value):
    loudness, own = 1.0, jax.random.fold_in(stream_key, 6)
    for position, shards_of in cuts:
        heights = jnp.exp(jax.random.uniform(jax.random.fold_in(own, position), (shards_of,), jnp.float32, low / len(cuts), top_value / len(cuts)))
        loudness = loudness * jnp.repeat(heights, extent[position] // shards_of).reshape([-1 if axis == position else 1 for axis in range(len(extent))])
    return loudness


def rank_table(amount, lean):
    portions = [(1 << 20) // math.isqrt(standing ** lean) + 1 for standing in range(1, amount + 1)]
    scale = 1 + sum(portions) // (1 << 30)
    return np.cumsum(np.array([max(1, weight // scale) for weight in portions]))


def ranked(stream_key, shape, amount, slope):
    table = rank_table(amount, slope)
    pick = jax.random.randint(jax.random.fold_in(stream_key, 1), shape, 0, int(table[amount - 1]))
    grade = jnp.searchsorted(jnp.asarray(table, jnp.int32), pick, side="right")
    return jax.random.permutation(jax.random.fold_in(stream_key, 2), amount)[grade].astype(jnp.int32)


def noise(own_key, extent, scale, limit, cuts=(), kind=jnp.bfloat16):
    drawn = jax.random.normal(own_key, extent, jnp.float32) * scale
    if len(cuts) > 0:
        drawn = steps_of(own_key, extent, cuts, -0.22, 0.18) * drawn
    return jnp.clip(drawn, min=-limit, max=limit).astype(kind)


def setup_inputs(seed: int = 0) -> dict:
    seeds = jax.random.split(jax.random.key(seed), 10)
    pooled_grad = noise(seeds[0], (B, NT, D), 1.0, 6.0, ((0, 32),))
    grad_scale = jnp.clip(jnp.exp(math.log(1.0) - 2.9996462 * jax.random.uniform(seeds[1], (B, NT), jnp.float32) ** steps_of(seeds[1], (B, NT), ((0, 32),), -0.2, 0.2)), 0.049804688, 1.0).astype(jnp.bfloat16)
    hot_slot = touch_ends(ranked(seeds[2], (B, NT, LH), HOT, 2), jax.random.fold_in(seeds[2], 3), 0, HOT - 1).astype(jnp.int32)
    send_index = draw_send_index(jax.random.fold_in(seeds[9], 71), 0)
    recv_row = draw_recv_row(jax.random.fold_in(seeds[9], 71), 0)
    cold_weight = noise(seeds[5], (NT, TABLE_ROWS, D), 0.5, 3.0, ((1, 32),), jnp.float32)
    cold_accum = jnp.clip(jnp.exp(math.log(8.0) - 2.7725887 * jax.random.uniform(seeds[6], (NT, TABLE_ROWS), jnp.float32) ** steps_of(seeds[6], (NT, TABLE_ROWS), ((1, 32),), -0.2, 0.2)), 0.5, 8.0)
    hot_weight = noise(seeds[7], (NT, HOT, D), 0.5, 3.0, (), jnp.float32)
    hot_accum = jnp.clip(jnp.exp(jax.random.uniform(seeds[8], (NT, HOT), jnp.float32, math.log(1.0), math.log(64.0))), 1.0, 64.0)
    return {"pooled_grad": pooled_grad, "grad_scale": grad_scale, "hot_slot": hot_slot, "send_index": send_index, "recv_row": recv_row, "cold_weight": cold_weight, "cold_accum": cold_accum, "hot_weight": hot_weight, "hot_accum": hot_accum}


LEARN_RATE = 0.5

def adagrad(weight, accum, grad):
    accum_new = accum + lax.optimization_barrier(jnp.mean(grad * grad, axis=-1))
    return (weight - LEARN_RATE * grad / jnp.sqrt(accum_new)[..., None], accum_new)

def reference(pooled_grad, grad_scale, hot_slot, send_index, recv_row, cold_weight, cold_accum, hot_weight, hot_accum):
    dequantized = pooled_grad.astype(jnp.float32) * grad_scale.astype(jnp.float32)[:, :, None]
    grad_rows = dequantized.reshape(B * NT, D)
    local_rows = NT * ROWS_DEV
    senders = jnp.arange(DEVICES, dtype=jnp.int32) * (B_DEV * NT)

    def owner_grad(owner):
        picked = lax.dynamic_index_in_dim(send_index, owner, 1, keepdims=False)
        source = (senders[:, None] + picked.astype(jnp.int32)).reshape(DEVICES * CAP)
        target = lax.dynamic_index_in_dim(recv_row, owner, 0, keepdims=False).reshape(DEVICES * CAP)
        values = jnp.take(grad_rows, source, axis=0)
        return jax.ops.segment_sum(values, target.astype(jnp.int32), num_segments=local_rows + 1)[:local_rows]
    owners = jnp.arange(DEVICES, dtype=jnp.int32)
    cold_grad = lax.map(owner_grad, owners)
    cold_grad = cold_grad.reshape(DEVICES, NT, ROWS_DEV, D).transpose(1, 0, 2, 3).reshape(NT, TABLE_ROWS, D)
    cold_weight_new, cold_accum_new = adagrad(cold_weight, cold_accum, cold_grad)
    table_base = (jnp.arange(NT, dtype=jnp.int32) * HOT)[None, :, None]
    hot_index = (hot_slot.astype(jnp.int32) + table_base).reshape(B * NT * LH)
    spread = jnp.broadcast_to(dequantized[:, :, None, :], (B, NT, LH, D)).reshape(B * NT * LH, D)
    hot_grad = jax.ops.segment_sum(spread, hot_index, num_segments=NT * HOT).reshape(NT, HOT, D)
    hot_weight_new, hot_accum_new = adagrad(hot_weight, hot_accum, hot_grad)
    return (cold_weight_new, cold_accum_new, hot_weight_new, hot_accum_new)
```

```python
import functools

import jax
import jax.numpy as jnp
from jax import lax
from jax.experimental import pallas as pl
from jax.experimental.pallas import tpu as pltpu
from jax.sharding import PartitionSpec as P

LEARN_RATE = 0.5
LANES = 128
AXES = ("node", "chip")


class Sizes:
    def __init__(self, pooled_grad, hot_slot, send_index, cold_weight, hot_weight):
        self.b_dev, self.tables, self.width = pooled_grad.shape
        self.hits = hot_slot.shape[2]
        self.devices, self.cap = send_index.shape[1:]
        self.rows_dev = cold_weight.shape[1]
        self.hot_rows = hot_weight.shape[1]
        self.source = self.b_dev * self.tables
        self.halves = self.width // LANES
        self.index_at = self.halves * self.source
        self.index_rows = self.devices * self.cap // LANES
        self.scale_at = self.index_at + self.index_rows
        self.lane_rows = self.source // LANES
        self.hot_at = self.scale_at + self.lane_rows
        used = self.hot_at + self.hits * self.lane_rows
        self.rows = -(-used // 16) * 16
        self.hot_shift = 256
        self.cold_total = self.tables * self.rows_dev
        self.hot_total = self.tables * self.hot_rows


def pack(z, pooled_grad, grad_scale, hot_slot, send_index):
    rows = pooled_grad.transpose(1, 0, 2).reshape(z.source, z.halves, LANES)
    rows = rows.transpose(1, 0, 2).reshape(z.index_at, LANES)
    sample_first = send_index.reshape(z.index_rows, LANES)
    table_first = (sample_first % z.tables) * z.b_dev + sample_first // z.tables
    scale = grad_scale.T.reshape(z.lane_rows, LANES)
    hot = hot_slot.transpose(2, 1, 0).reshape(z.hits * z.lane_rows, LANES) - z.hot_shift
    pad = z.rows - z.hot_at - z.hits * z.lane_rows
    parts = [rows, table_first.astype(jnp.bfloat16), scale, hot.astype(jnp.bfloat16)]
    if pad:
        parts.append(jnp.zeros((pad, LANES), jnp.bfloat16))
    return jnp.concatenate(parts, axis=0)


def device_index(chips):
    return lax.axis_index("node") * chips + lax.axis_index("chip")


def unit_prep(z, me, sender, unit, recv_ref, target_s, scale_s, picked_s, at):
    cap, source = z.cap, z.source
    index_rows = unit[z.index_at : z.index_at + z.index_rows, :].astype(jnp.float32)
    row_of = lax.broadcasted_iota(jnp.int32, index_rows.shape, 0)
    mine = jnp.sum(
        jnp.where(row_of == (me * cap) // LANES, index_rows, 0.0), axis=0, keepdims=True
    )
    if cap < LANES:
        mine = pltpu.roll(
            jnp.broadcast_to(mine, (8, LANES)), lax.rem(LANES - lax.rem(me * cap, LANES), LANES), 1
        )[:1]
    column = jnp.broadcast_to(mine, (LANES, LANES)).T[:cap]
    lane = lax.broadcasted_iota(jnp.int32, (cap, LANES), 1).astype(jnp.float32)
    onehot = jnp.concatenate(
        [
            jnp.where(column == lane + float(h * LANES), 1.0, 0.0).astype(jnp.bfloat16)
            for h in range(source // LANES)
        ],
        axis=1,
    )
    rows = jnp.concatenate(
        [unit[h * source : (h + 1) * source, :] for h in range(z.halves)], axis=1
    )
    picked_s[at * cap : (at + 1) * cap, :] = jnp.dot(
        onehot, rows, preferred_element_type=jnp.float32
    ).astype(jnp.bfloat16)
    scale = unit[z.scale_at : z.scale_at + z.lane_rows, :]
    scale = jnp.concatenate(
        [jnp.broadcast_to(scale[r : r + 1], (16, LANES)) for r in range(z.lane_rows)], axis=1
    )
    chosen = lax.dot_general(
        scale, onehot, (((1,), (1,)), ((), ())), preferred_element_type=jnp.float32
    )
    scale_s[:, at * cap : (at + 1) * cap] = chosen[:8]
    target_s[:, at * cap : (at + 1) * cap] = jnp.broadcast_to(recv_ref[pl.ds(sender, 1), :], (8, cap))


def add_cold(z, count, target_s, scale_s, picked_s, acc_ref, first, block, depth):
    for k0 in range(0, count * z.cap, depth):
        target = target_s[:1, k0 : k0 + depth]
        scale = scale_s[:1, k0 : k0 + depth]
        picked = picked_s[k0 : k0 + depth, :]

        def body(i, carry):
            start = pl.multiple_of(i * block, block)
            level = lax.broadcasted_iota(jnp.int32, (block, depth), 0) + start
            weights = jnp.where(level == target, scale, 0.0).astype(jnp.bfloat16)
            term = jnp.dot(weights, picked, preferred_element_type=jnp.float32)
            if first and k0 == 0:
                acc_ref[pl.ds(start, block), :] = term
            else:
                acc_ref[pl.ds(start, block), :] += term
            return carry

        lax.fori_loop(0, z.cold_total // block, body, 0)


def add_hot(z, units, acc_ref, first):
    b_dev = z.b_dev
    for t in range(z.tables):
        row, col = divmod(t * b_dev, LANES)
        pieces = []
        for unit in units:
            pieces.append(
                jnp.concatenate(
                    [
                        unit[h * z.source + t * b_dev : h * z.source + (t + 1) * b_dev, :]
                        for h in range(z.halves)
                    ],
                    axis=1,
                )
            )
        rows = jnp.concatenate(pieces, axis=0)

        def lanes(at):
            return jnp.concatenate(
                [unit[at + row : at + row + 1, col : col + b_dev].astype(jnp.float32) for unit in units],
                axis=1,
            )

        scale = lanes(z.scale_at)
        level = lax.broadcasted_iota(jnp.int32, (z.hot_rows, len(units) * b_dev), 0).astype(jnp.float32)
        coeff = None
        for l in range(z.hits):
            slot = lanes(z.hot_at + l * z.lane_rows) + float(z.hot_shift)
            term = jnp.where(level == slot, scale, 0.0)
            coeff = term if coeff is None else coeff + term
        term = jnp.dot(coeff.astype(jnp.bfloat16), rows, preferred_element_type=jnp.float32)
        where = slice(t * z.hot_rows, (t + 1) * z.hot_rows)
        if first:
            acc_ref[where, :] = term
        else:
            acc_ref[where, :] += term


def adagrad(grad_ref, weight_ref, accum_ref, weight_out, accum_out, width):
    rows = grad_ref.shape[0]
    same = lax.broadcasted_iota(jnp.int32, (LANES, LANES), 0) == lax.broadcasted_iota(
        jnp.int32, (LANES, LANES), 1
    )

    def body(i, carry):
        start = pl.multiple_of(i * LANES, LANES)
        grad = grad_ref[pl.ds(start, LANES), :]
        square = grad * grad
        total = square[:, :LANES]
        for h in range(1, width // LANES):
            total = total + square[:, h * LANES : (h + 1) * LANES]
        old = jnp.broadcast_to(accum_ref[pl.ds(i, 1), :], (LANES, LANES))
        mean = jnp.sum(total, axis=1, keepdims=True) * (1.0 / width)
        new = jnp.sum(jnp.where(same, old, 0.0), axis=1, keepdims=True) + mean
        weight_out[pl.ds(start, LANES), :] = (
            weight_ref[pl.ds(start, LANES), :] - LEARN_RATE * grad * lax.rsqrt(new)
        )
        accum_out[pl.ds(i, 1), :] = jnp.sum(jnp.where(same, new, 0.0), axis=0, keepdims=True)
        return carry

    lax.fori_loop(0, rows // LANES, body, 0)


def sender_of(me, offsets, j):
    return me ^ jnp.where(me % 2 == 0, offsets[0][j], offsets[1][j])


def reduce_kernel(z, chips, offsets, first, counts, *refs):
    *groups, recv_ref, refs_rest = refs[: len(counts)], refs[len(counts)], refs[len(counts) + 1 :]
    groups = groups[0]
    if first:
        cold_acc, hot_acc, target_s, scale_s, picked_s = refs_rest
    else:
        _, _, cold_acc, hot_acc, target_s, scale_s, picked_s = refs_rest
    me = device_index(chips)
    units = [group.at[j] for group, n in zip(groups, counts) for j in range(n)]
    for j, unit in enumerate(units):
        unit_prep(z, me, sender_of(me, offsets, j), unit, recv_ref, target_s, scale_s, picked_s, j)
    add_cold(z, len(units), target_s, scale_s, picked_s, cold_acc, first, min(1024, z.cold_total), min(512, len(units) * z.cap))
    for j in range(0, len(units), 4):
        add_hot(z, units[j : j + 4], hot_acc, first and j == 0)


def call_reduce(z, chips, groups, offsets, recv, accs):
    counts = [g.shape[0] for g in groups]
    slots = sum(counts) * z.cap
    first = accs is None
    vmem = pl.BlockSpec(memory_space=pltpu.VMEM)
    args = [*groups, recv] + ([] if first else list(accs))
    return pl.pallas_call(
        functools.partial(reduce_kernel, z, chips, offsets, first, counts),
        out_shape=(
            pltpu.VMEM((z.cold_total, z.width), jnp.float32),
            pltpu.VMEM((z.hot_total, z.width), jnp.float32),
        ),
        in_specs=[vmem] * len(args),
        out_specs=(vmem, vmem),
        scratch_shapes=[
            pltpu.VMEM((8, slots), jnp.int32),
            pltpu.VMEM((8, slots), jnp.float32),
            pltpu.VMEM((slots, z.width), jnp.bfloat16),
        ],
        input_output_aliases={} if first else {len(args) - 2: 0, len(args) - 1: 1},
        compiler_params=pltpu.CompilerParams(vmem_limit_bytes=24 * 2**20),
        cost_estimate=pl.CostEstimate(
            flops=2 * slots * z.cold_total * z.width, bytes_accessed=2**20, transcendentals=0
        ),
    )(*args)


def update_kernel(width, grad_ref, weight_ref, accum_ref, weight_out, accum_out):
    adagrad(grad_ref, weight_ref, accum_ref, weight_out, accum_out, width)


def call_update(grad, weight, accum):
    rows, width = grad.shape
    block = min(1024, rows)
    return pl.pallas_call(
        functools.partial(update_kernel, width),
        grid=(rows // block,),
        out_shape=(
            jax.ShapeDtypeStruct((rows, width), jnp.float32),
            jax.ShapeDtypeStruct((rows // LANES, LANES), jnp.float32),
        ),
        in_specs=[
            pl.BlockSpec((block, width), lambda i: (i, 0)),
            pl.BlockSpec((block, width), lambda i: (i, 0)),
            pl.BlockSpec((block // LANES, LANES), lambda i: (i, 0)),
        ],
        out_specs=(
            pl.BlockSpec((block, width), lambda i: (i, 0)),
            pl.BlockSpec((block // LANES, LANES), lambda i: (i, 0)),
        ),
    )(grad, weight, accum)


def per_device(
    nodes,
    chips,
    pooled_grad,
    grad_scale,
    hot_slot,
    send_index,
    recv_row,
    cold_weight,
    cold_accum,
    hot_weight,
    hot_accum,
):
    z = Sizes(pooled_grad, hot_slot, send_index, cold_weight, hot_weight)
    bits = chips.bit_length() - 1
    turn = (bits - 1) // 2

    def swap(x, flip):
        return lax.ppermute(x, AXES, [(i, i ^ flip(i % 2)) for i in range(nodes * chips)])

    mine = pack(z, pooled_grad, grad_scale, hot_slot, send_index)
    recv = recv_row.reshape(z.devices, z.cap)
    far = {k: swap(mine, lambda core, k=k: k * chips) for k in range(nodes - 1, 0, -1)}
    groups = [[0, 1], list(range(2, nodes))]
    accs = None
    for near in groups:
        held = jnp.stack([mine if k == 0 else far[k] for k in near])
        offsets = [[k * chips for k in near]] * 2
        for step in range(bits - 1):
            flips = [1 << (1 + step), 1 << (1 + (step + turn) % (bits - 1))]
            other = swap(held, lambda core: flips[core])
            held = jnp.concatenate([held, other])
            offsets = [o + [k ^ f for k in o] for o, f in zip(offsets, flips)]
        other = swap(held, lambda core: 1)
        accs = call_reduce(z, chips, [held], offsets, recv, accs)
        offsets = [[k ^ 1 for k in offsets[1]], [k ^ 1 for k in offsets[0]]]
        accs = call_reduce(z, chips, [other], offsets, recv, accs)
    cold, hot = accs
    new_weight, new_accum = call_update(
        cold, cold_weight.reshape(z.cold_total, z.width), cold_accum.reshape(-1, LANES)
    )
    hot_new, hot_accum_new = call_update(
        hot, hot_weight.reshape(z.hot_total, z.width), hot_accum.reshape(-1, LANES)
    )
    return (
        new_weight.reshape(cold_weight.shape),
        new_accum.reshape(cold_accum.shape),
        hot_new.reshape(hot_weight.shape),
        hot_accum_new.reshape(hot_accum.shape),
    )


def solution(mesh):
    placed = (
        P(AXES, None, None),
        P(AXES, None),
        P(AXES, None, None),
        P(AXES, None, None),
        P(AXES, None, None),
        P(None, AXES, None),
        P(None, AXES),
        P(),
        P(),
    )
    return jax.shard_map(
        functools.partial(per_device, mesh.shape["node"], mesh.shape["chip"]),
        mesh=mesh,
        in_specs=placed,
        out_specs=(P(None, AXES, None), P(None, AXES), P(), P()),
        check_vma=False,
    )
```
